32 devices in a mesh: dp: 4 (over z), mp: 4 (over y, x), mc: 2 (over core).
Axes of the slice: x: 2, y: 2, z: 4, core: 2. Of those that a mesh axis runs over, the one named last changes fastest.
Arguments:
- features: bfloat16 [1576, 768], P('dp'), may hold values from -6 to 6
- out_cotangent: bfloat16 [2, 1576, 768], P('mc', 'dp'), may hold values from -6 to 6
- mean_up: float32 [768, 3072], P('dp', 'mp'), may hold values from -0.21875 to 0.21875
- precision_up: float32 [768, 3072], P('dp', 'mp'), may hold values from 4 to 64
- noise_up: float32 [2, 768, 3072], P('mc', 'dp', 'mp'), may hold values from -6 to 6
- mean_down: float32 [768, 3072], P('dp', 'mp'), may hold values from -0.109375 to 0.109375
- precision_down: float32 [768, 3072], P('dp', 'mp'), may hold values from 4 to 64
- noise_down: float32 [2, 768, 3072], P('mc', 'dp', 'mp'), may hold values from -6 to 6
Outputs:
- mean_new_up: float32 [768, 3072], P('dp', 'mp')
- precision_new_up: float32 [768, 3072], P('dp', 'mp')
- mean_new_down: float32 [768, 3072], P('dp', 'mp')
- precision_new_down: float32 [768, 3072], P('dp', 'mp')
- input_grad: bfloat16 [2, 1576, 768], P('mc', 'dp', 'mp')
The draws below stay inside these ranges and needn't reach their ends.
All inputs are finite; a program needn't handle non-finite values.
Results may differ from the reference program's by a relative error of at most 0.0015.
The reference program's roundings to bfloat16 on the way (of `hidden` and `preact_grad`) count: a program that leaves them out, or rounds other values in their place, can miss the bound.
Values may be sent and summed in bfloat16 or wider, within the bound.
No kernel may reach another device: no remote copies, remote signals or barrier semaphores. Data moves between devices by JAX's collectives and lax.ppermute only.
A program may use at most 64 MiB of HBM per device.

```python
import math
import jax
import jax.numpy as jnp
from jax import lax

D = 768
FF = 3072
PATCHES = 197
MC = 2
IMAGES = 8
TOKENS = 1576


def raised(result, key, source, target, blocks, factor):
    def block_of(axis_at):
        return (jnp.arange(result.shape[axis_at]) // (result.shape[axis_at] // blocks)).reshape((-1,) + (1,) * (result.ndim - 1 - axis_at))

    one_side = jax.random.permutation(key, blocks)[block_of(target)]
    other_side = (block_of(target) + blocks // 2) % blocks
    return jnp.where((block_of(source) == one_side) | (block_of(source) == other_side), factor * result, result)


def block_scale(rng, extent, cuts, low, largest):
    level, own = 1.0, jax.random.fold_in(rng, 6)
    for position, shards_of in cuts:
        steps = jnp.exp(jax.random.uniform(jax.random.fold_in(own, position), (shards_of,), jnp.float32, low / len(cuts), largest / len(cuts)))
        level = level * jnp.repeat(steps, extent[position] // shards_of).reshape([-1 if axis == position else 1 for axis in range(len(extent))])
    return level


def scatter_about(stream_key, dims, width, limit, split=(), held_as=jnp.bfloat16):
    drawn = width * jax.random.normal(stream_key, dims, jnp.float32)
    if split:
        drawn = drawn * block_scale(stream_key, dims, split, -0.22, 0.18)
    return jnp.clip(drawn, -limit, limit).astype(held_as)


def bell_draw_with(own_key, extent, scale, bound, split, heavy, dtype=jnp.bfloat16):
    values = scale * jax.random.normal(own_key, extent, jnp.float32)
    if split:
        values = values * block_scale(own_key, extent, split, -0.22, 0.18)
    return jnp.clip(raised(values, jax.random.fold_in(own_key, 3), *heavy), -bound, bound).astype(dtype)


def setup_inputs(seed: int = 0) -> dict:
    key_list = jax.random.split(jax.random.key(seed), 9)
    return {
        "features": bell_draw_with(key_list[0], (TOKENS, D), 1.0, 6.0, ((0, 4),), (0, 1, 4, 2.0)),
        "out_cotangent": bell_draw_with(key_list[1], (MC, TOKENS, D), 1.0, 6.0, ((0, 2), (1, 4)), (1, 2, 4, 2.0)),
        "mean_up": scatter_about(key_list[2], (D, FF), D ** -0.5, 0.21875, ((0, 4), (1, 4)), jnp.float32),
        "precision_up": jnp.clip(jnp.exp(math.log(64.0) - 2.7725887 * jax.random.uniform(key_list[3], (D, FF), jnp.float32) ** block_scale(key_list[3], (D, FF), ((0, 4), (1, 4)), -0.2, 0.2)), 4.0, 64.0),
        "noise_up": scatter_about(key_list[4], (MC, D, FF), 1.0, 6.0, ((0, 2), (1, 4), (2, 4)), jnp.float32),
        "mean_down": scatter_about(key_list[5], (D, FF), FF ** -0.5, 0.109375, ((0, 4), (1, 4)), jnp.float32),
        "precision_down": jnp.clip(jnp.exp(math.log(64.0) - 2.7725887 * jax.random.uniform(key_list[6], (D, FF), jnp.float32) ** block_scale(key_list[6], (D, FF), ((0, 4), (1, 4)), -0.2, 0.2)), 4.0, 64.0),
        "noise_down": scatter_about(key_list[7], (MC, D, FF), 1.0, 6.0, ((0, 2), (1, 4), (2, 4)), jnp.float32),
    }


reciprocal_root = 0.7071067811865476
normal_peak = 0.3989422804014327
tempering = 100.0
damping = 4.0
average_rate = 0.25
step_rate = 0.05
clip_level = 0.01

def gelu_parts(preact):
    cumulative = 0.5 * (1.0 + lax.erf(preact * reciprocal_root))
    density = normal_peak * jnp.exp(-0.5 * preact * preact)
    return (preact * cumulative, cumulative + preact * density)

def sample_weights(center, precision, noise_draw):
    spread = 1.0 / jnp.sqrt(tempering * (precision + damping))
    return (center + spread * noise_draw).astype(jnp.bfloat16)

def contract_rows(left, right):
    return lax.dot_general(left, right, (((0,), (0,)), ((), ())), preferred_element_type=jnp.float32)

def contract_cols(left, right):
    return lax.dot_general(left, right, (((1,), (1,)), ((), ())), preferred_element_type=jnp.float32)

def reference(features, out_cotangent, mean_up, precision_up, noise_up, mean_down, precision_down, noise_down):
    images = features.shape[0] // PATCHES
    pictures = features.reshape(images, PATCHES, D)
    empty_sum = jnp.zeros((D, FF), jnp.float32)
    running = (empty_sum, empty_sum, empty_sum, empty_sum)
    gradients = []
    for sample_index in range(MC):
        w_up = sample_weights(mean_up, precision_up, noise_up[sample_index])
        w_down = sample_weights(mean_down, precision_down, noise_down[sample_index])
        cotangent = out_cotangent[sample_index].reshape(images, PATCHES, D)

        def per_image(totals, image_pair):
            image_rows, cotangent_rows = image_pair
            preact = jnp.dot(image_rows, w_up, preferred_element_type=jnp.float32)
            gelu_value, gelu_slope = gelu_parts(preact)
            hidden = gelu_value.astype(jnp.bfloat16)
            hidden_grad = jnp.dot(cotangent_rows, w_down, preferred_element_type=jnp.float32)
            preact_grad = (hidden_grad * gelu_slope).astype(jnp.bfloat16)
            input_rows = contract_cols(preact_grad, w_up).astype(jnp.bfloat16)
            grad_up = contract_rows(image_rows, preact_grad)
            grad_down = contract_rows(cotangent_rows, hidden)
            updated = (totals[0] + grad_up, totals[1] + grad_up * grad_up, totals[2] + grad_down, totals[3] + grad_down * grad_down)
            return (updated, input_rows)
        running, input_rows = lax.scan(per_image, running, (pictures, cotangent))
        gradients.append(input_rows.reshape(images * PATCHES, D))
    input_grad = jnp.stack(gradients)
    grad_up = running[0] / MC
    square_up = running[1] / (MC * IMAGES)
    grad_down = running[2] / MC
    square_down = running[3] / (MC * IMAGES)
    precision_new_up = (1.0 - average_rate) * precision_up + average_rate * square_up
    precision_new_down = (1.0 - average_rate) * precision_down + average_rate * square_down
    raw_up = grad_up / (precision_new_up + damping)
    raw_down = grad_down / (precision_new_down + damping)
    global_sum = jnp.sum(raw_up * raw_up) + jnp.sum(raw_down * raw_down)
    root_mean = jnp.sqrt(global_sum / (2 * D * FF))
    factor = 1.0 / jnp.maximum(clip_level, root_mean)
    mean_new_up = mean_up - step_rate * factor * raw_up
    mean_new_down = mean_down - step_rate * factor * raw_down
    return (mean_new_up, precision_new_up, mean_new_down, precision_new_down, input_grad)
```

```python
import functools
import jax
import jax.numpy as jnp
from jax import lax
from jax.experimental import pallas as pl
from jax.experimental.pallas import tpu as pltpu
from jax.sharding import PartitionSpec as P

PATCHES = 197
SLOT = 208


reciprocal_root = 0.7071067811865476
normal_peak = 0.3989422804014327
tempering = 100.0
damping = 4.0
average_rate = 0.25
step_rate = 0.05
clip_level = 0.01


def gelu_parts(preact):
    cumulative = 0.5 * (1.0 + lax.erf(preact * reciprocal_root))
    density = normal_peak * jnp.exp(-0.5 * preact * preact)
    return (preact * cumulative, cumulative + preact * density)


def sample_weights(center, precision, noise_draw):
    spread = 1.0 / jnp.sqrt(tempering * (precision + damping))
    return (center + spread * noise_draw).astype(jnp.bfloat16)


def contract_rows(left, right):
    return lax.dot_general(
        left, right, (((0,), (0,)), ((), ())), preferred_element_type=jnp.float32
    )


def contract_cols(left, right):
    return lax.dot_general(
        left, right, (((1,), (1,)), ((), ())), preferred_element_type=jnp.float32
    )


def shards_general(
    features, out_cotangent, mean_up, precision_up, noise_up, mean_down, precision_down, noise_down
):
    w_up = lax.all_gather(sample_weights(mean_up, precision_up, noise_up[0]), "dp", axis=0, tiled=True)
    w_down = lax.all_gather(
        sample_weights(mean_down, precision_down, noise_down[0]), "dp", axis=0, tiled=True
    )
    cotangent = out_cotangent[0]
    preact = jnp.dot(features, w_up, preferred_element_type=jnp.float32)
    gelu_value, gelu_slope = gelu_parts(preact)
    hidden = gelu_value.astype(jnp.bfloat16)
    hidden_grad = jnp.dot(cotangent, w_down, preferred_element_type=jnp.float32)
    preact_grad = (hidden_grad * gelu_slope).astype(jnp.bfloat16)
    partial_value = contract_cols(preact_grad, w_up)
    input_grad = lax.psum_scatter(partial_value, "mp", scatter_dimension=1, tiled=True).astype(
        jnp.bfloat16
    )[None]
    images = features.shape[0] // PATCHES
    totals = [jnp.zeros(w_up.shape, jnp.float32)] * 4
    for image in range(images):
        rows = slice(image * PATCHES, (image + 1) * PATCHES)
        grad_up = contract_rows(features[rows], preact_grad[rows])
        grad_down = contract_rows(cotangent[rows], hidden[rows])
        terms = (grad_up, grad_up * grad_up, grad_down, grad_down * grad_down)
        totals = [total + term for total, term in zip(totals, terms)]
    totals = [lax.psum_scatter(t, "dp", scatter_dimension=0, tiled=True) for t in totals]
    totals = lax.psum(tuple(totals), "mc")
    samples = lax.axis_size("mc")
    images_all = images * lax.axis_size("dp")
    raws, news = [], []
    for (grad, square), precision in zip(
        (totals[:2], totals[2:]), (precision_up, precision_down)
    ):
        new, raw = update(grad, square, precision, samples, images_all)
        raws.append(raw)
        news.append(new)
    entries = 2 * raws[0].size * lax.axis_size("dp") * lax.axis_size("mp")
    local_sum = jnp.sum(raws[0] * raws[0]) + jnp.sum(raws[1] * raws[1])
    scale = step_scale(lax.psum(local_sum, ("dp", "mp")), entries)
    return (mean_up - scale * raws[0], news[0], mean_down - scale * raws[1], news[1], input_grad)


def update(grad_sum, square_sum, precision, samples, images_all):
    square = square_sum / (samples * images_all)
    new = (1.0 - average_rate) * precision + average_rate * square
    return new, (grad_sum / samples) / (new + damping)


def step_scale(global_sum, entries):
    root_mean = jnp.sqrt(global_sum / entries)
    return step_rate * (1.0 / jnp.maximum(clip_level, root_mean))


def swap_core(value):
    return lax.ppermute(value, "mc", [(0, 1), (1, 0)])


def swap_bit(value, axis, bit):
    size = lax.axis_size(axis)
    return lax.ppermute(value, axis, [(j, j ^ bit) for j in range(size)])


def gather_line(blocks, n):
    me = lax.axis_index("dp")
    above = [{} for _ in blocks]
    below = [{} for _ in blocks]
    for stage in range(1, n):
        up = [(j, j + 1) for j in range(stage - 1, n - 1)]
        down = [(n - 1 - a, n - 1 - b) for a, b in up]
        for at, block in enumerate(blocks):
            below[at][stage] = lax.ppermute(below[at].get(stage - 1, block), "dp", up)
            above[at][stage] = lax.ppermute(above[at].get(stage - 1, block), "dp", down)
    return [
        [block] + [jnp.where(me + k < n, above[at][k], below[at][n - k]) for k in range(1, n)]
        for at, block in enumerate(blocks)
    ]


def scatter_line(parts, n):
    rows = parts[0].shape[0] // n
    block = lambda part, k: part[k * rows : (k + 1) * rows]
    ups = [None] * len(parts)
    downs = [None] * len(parts)
    for stage in range(1, n):
        up = [(j, j + 1) for j in range(stage)]
        down = [(n - 1 - a, n - 1 - b) for a, b in up]
        for at, part in enumerate(parts):
            send_up, send_down = block(part, n - stage), block(part, stage)
            if stage > 1:
                send_up = (send_up + ups[at].astype(jnp.float32))
                send_down = (send_down + downs[at].astype(jnp.float32))
            ups[at] = lax.ppermute(send_up, "dp", up)
            downs[at] = lax.ppermute(send_down, "dp", down)
    return [block(part, 0) + up + down for part, up, down in zip(parts, ups, downs)]


def sums_kernel(images, slot, left_own, left_other, right_own, right_other, grad_ref, square_ref):
    def block(at, carry):
        columns = pl.ds(pl.multiple_of(at * 128, 128), 128)
        total = None
        for left, right in ((left_own, right_own), (left_other, right_other)):
            for image in range(images):
                rows = pl.ds(image * slot, slot)
                one = contract_rows(left[rows, columns], right[rows, :])
                if total is None:
                    total, squares = one, one * one
                else:
                    total, squares = total + one, squares + one * one
        grad_ref[columns, :] = total
        square_ref[columns, :] = squares
        return carry

    lax.fori_loop(0, grad_ref.shape[0] // 128, block, 0)


def image_sums(left_own, left_other, right_own, right_other, images, slot):
    shape = (left_own.shape[1], right_own.shape[1])
    flops = 4 * images * slot * shape[0] * shape[1]
    vmem = pl.BlockSpec(memory_space=pltpu.VMEM)
    return pl.pallas_call(
        functools.partial(sums_kernel, images, slot),
        out_shape=[jax.ShapeDtypeStruct(shape, jnp.float32)] * 2,
        in_specs=[vmem] * 4,
        out_specs=[vmem] * 2,
        cost_estimate=pl.CostEstimate(
            flops=flops, bytes_accessed=8 * shape[0] * shape[1] * 2, transcendentals=0
        ),
        name="image_sums",
    )(left_own, left_other, right_own, right_other)


def pad_images(value, images, slot):
    value = value.reshape(images, PATCHES, value.shape[-1])
    return jnp.pad(value, ((0, 0), (0, slot - PATCHES), (0, 0))).reshape(images * slot, -1)


def all_sum(value, axes):
    for axis in axes:
        bit = 1
        while bit < lax.axis_size(axis):
            value = value + swap_bit(value, axis, bit)
            bit *= 2
    return value


def shards_line(
    features, out_cotangent, mean_up, precision_up, noise_up, mean_down, precision_down, noise_down
):
    n = lax.axis_size("dp")
    me, place, core = lax.axis_index("dp"), lax.axis_index("mp"), lax.axis_index("mc")
    images = features.shape[0] // PATCHES
    slot = SLOT
    rows, width = mean_up.shape
    half = width // 2
    shard_up = sample_weights(mean_up, precision_up, noise_up[0])
    shard_down = sample_weights(mean_down, precision_down, noise_down[0])

    def rotated(value):
        return lax.dynamic_slice_in_dim(
            jnp.concatenate([value, value], 1), me * rows, value.shape[1], 1
        )

    feats = pad_images(rotated(features), images, slot)
    cot = pad_images(rotated(out_cotangent[0]), images, slot)
    cot_other = swap_core(cot)

    up_parts = gather_line([shard_up[:, :half], shard_up[:, half:]], n)
    w_up = jnp.concatenate([jnp.concatenate(part, 0) for part in up_parts], 1)
    down_parts = gather_line([shard_down[:, :half], shard_down[:, half:]], n)
    w_down = jnp.concatenate([jnp.concatenate(part, 0) for part in down_parts], 1)

    def split(value):
        keep = lax.dynamic_slice_in_dim(value, core * half, half, 1)
        send = lax.dynamic_slice_in_dim(value, (1 - core) * half, half, 1)
        return keep, swap_core(send)

    preact = jnp.dot(feats, w_up, preferred_element_type=jnp.float32)
    gelu_value, gelu_slope = gelu_parts(preact)
    hidden_own, hidden_other = split(gelu_value.astype(jnp.bfloat16))
    sums_down = image_sums(cot, cot_other, hidden_own, hidden_other, images, slot)
    totals_down = scatter_line(sums_down, n)

    hidden_grad = jnp.dot(cot, w_down, preferred_element_type=jnp.float32)
    preact_grad = (hidden_grad * gelu_slope).astype(jnp.bfloat16)
    grad_own, grad_other = split(preact_grad)
    sums_up = image_sums(feats, feats, grad_own, grad_other, images, slot)
    totals_up = scatter_line(sums_up, n)

    quarters = []
    for k in range(4):
        at = lax.rem((place ^ k) + n - me, n)
        quarters.append(
            contract_cols(preact_grad, lax.dynamic_slice_in_dim(w_up, at * rows, rows, 0))
        )
    far = swap_bit(jnp.stack([quarters[2], quarters[3]]), "mp", 2)
    near = swap_bit(quarters[1] + far[1], "mp", 1)
    input_grad = (quarters[0] + far[0] + near).astype(jnp.bfloat16)
    input_grad = input_grad.reshape(images, slot, rows)[:, :PATCHES].reshape(1, -1, rows)

    samples = lax.axis_size("mc")
    images_all = images * n

    def own_half(value):
        return lax.dynamic_slice_in_dim(value, core * half, half, 1)

    new_up, raw_up = update(*totals_up, own_half(precision_up), samples, images_all)
    new_down, raw_down = update(*totals_down, own_half(precision_down), samples, images_all)
    local_sum = jnp.sum(raw_up * raw_up) + jnp.sum(raw_down * raw_down)
    global_sum = all_sum(jnp.full((1, 128), local_sum), ("mc", "mp", "dp"))[0, 0]
    scale = step_scale(global_sum, 2 * rows * width * n * lax.axis_size("mp"))
    mine = jnp.stack([new_up, raw_up, new_down, raw_down])
    other = swap_core(mine)
    both = jnp.where(
        core == 0, jnp.concatenate([mine, other], 2), jnp.concatenate([other, mine], 2)
    )
    return (mean_up - scale * both[1], both[0], mean_down - scale * both[3], both[2], input_grad)


def solution(mesh):
    in_specs = (
        P("dp", None),
        P("mc", "dp", None),
        P("dp", "mp"),
        P("dp", "mp"),
        P("mc", "dp", "mp"),
        P("dp", "mp"),
        P("dp", "mp"),
        P("mc", "dp", "mp"),
    )
    out_specs = (P("dp", "mp"), P("dp", "mp"), P("dp", "mp"), P("dp", "mp"), P("mc", "dp", "mp"))
    sizes = mesh.shape
    line = sizes["dp"] == 4 and sizes["mp"] == 4 and sizes["mc"] == 2
    body = shards_line if line else shards_general
    return jax.shard_map(body, mesh=mesh, in_specs=in_specs, out_specs=out_specs, check_vma=False)
```

```python
import functools
import jax
import jax.numpy as jnp
from jax import lax
from jax.experimental import pallas as pl
from jax.experimental.pallas import tpu as pltpu
from jax.sharding import PartitionSpec as P


PATCHES = 197
SLOT = 208
DEPTH = 256


reciprocal_root = 0.7071067811865476
normal_peak = 0.3989422804014327
tempering = 100.0
damping = 4.0
average_rate = 0.25
step_rate = 0.05
clip_level = 0.01


def gelu_parts(preact):
    cumulative = 0.5 * (1.0 + lax.erf(preact * reciprocal_root))
    density = normal_peak * jnp.exp(-0.5 * preact * preact)
    return (preact * cumulative, cumulative + preact * density)


def sample_weights(center, precision, noise_draw):
    spread = 1.0 / jnp.sqrt(tempering * (precision + damping))
    return (center + spread * noise_draw).astype(jnp.bfloat16)


def contract_rows(left, right):
    return lax.dot_general(
        left, right, (((0,), (0,)), ((), ())), preferred_element_type=jnp.float32
    )


def contract_cols(left, right):
    return lax.dot_general(
        left, right, (((1,), (1,)), ((), ())), preferred_element_type=jnp.float32
    )


def shards_general(
    features, out_cotangent, mean_up, precision_up, noise_up, mean_down, precision_down, noise_down
):
    w_up = lax.all_gather(sample_weights(mean_up, precision_up, noise_up[0]), "dp", axis=0, tiled=True)
    w_down = lax.all_gather(
        sample_weights(mean_down, precision_down, noise_down[0]), "dp", axis=0, tiled=True
    )
    cotangent = out_cotangent[0]
    preact = jnp.dot(features, w_up, preferred_element_type=jnp.float32)
    gelu_value, gelu_slope = gelu_parts(preact)
    hidden = gelu_value.astype(jnp.bfloat16)
    hidden_grad = jnp.dot(cotangent, w_down, preferred_element_type=jnp.float32)
    preact_grad = (hidden_grad * gelu_slope).astype(jnp.bfloat16)
    partial_value = contract_cols(preact_grad, w_up)
    input_grad = lax.psum_scatter(partial_value, "mp", scatter_dimension=1, tiled=True).astype(
        jnp.bfloat16
    )[None]
    images = features.shape[0] // PATCHES
    totals = [jnp.zeros(w_up.shape, jnp.float32)] * 4
    for image in range(images):
        rows = slice(image * PATCHES, (image + 1) * PATCHES)
        grad_up = contract_rows(features[rows], preact_grad[rows])
        grad_down = contract_rows(cotangent[rows], hidden[rows])
        terms = (grad_up, grad_up * grad_up, grad_down, grad_down * grad_down)
        totals = [total + term for total, term in zip(totals, terms)]
    totals = [lax.psum_scatter(t, "dp", scatter_dimension=0, tiled=True) for t in totals]
    totals = lax.psum(tuple(totals), "mc")
    samples = lax.axis_size("mc")
    images_all = images * lax.axis_size("dp")
    raws, news = [], []
    for (grad, square), precision in zip(
        (totals[:2], totals[2:]), (precision_up, precision_down)
    ):
        new, raw = update(grad, square, precision, samples, images_all)
        raws.append(raw)
        news.append(new)
    entries = 2 * raws[0].size * lax.axis_size("dp") * lax.axis_size("mp")
    local_sum = jnp.sum(raws[0] * raws[0]) + jnp.sum(raws[1] * raws[1])
    scale = step_scale(lax.psum(local_sum, ("dp", "mp")), entries)
    return (mean_up - scale * raws[0], news[0], mean_down - scale * raws[1], news[1], input_grad)


def precision_update(precision, square):
    return (1.0 - average_rate) * precision + average_rate * square


def update(grad_sum, square_sum, precision, samples, images_all):
    new = precision_update(precision, square_sum / (samples * images_all))
    return new, (grad_sum / samples) / (new + damping)


def step_scale(global_sum, entries):
    root_mean = jnp.sqrt(global_sum / entries)
    return step_rate * (1.0 / jnp.maximum(clip_level, root_mean))


def swap_core(value):
    return lax.ppermute(value, "mc", [(0, 1), (1, 0)])


def swap_bit(value, axis, bit):
    size = lax.axis_size(axis)
    return lax.ppermute(value, axis, [(j, j ^ bit) for j in range(size)])


def exchange_one(value):
    return swap_bit(value, "dp", 1)


def exchange_two(value):
    last, cores = lax.axis_size("dp") - 1, lax.axis_size("mc")
    pairs = []
    for j in range(last + 1):
        for core in range(cores):
            to = (j, 1 - core) if j in (0, last) else (((j - 1) ^ 1) + 1, core)
            pairs.append((j * cores + core, to[0] * cores + to[1]))
    return lax.ppermute(value, ("dp", "mc"), pairs)


def slots(value, size):
    me = lax.axis_index("dp")
    blocks = [value[:, k * size : (k + 1) * size] for k in range(lax.axis_size("dp"))]
    bit = 1
    while bit < len(blocks):
        blocks = [jnp.where(me & bit, blocks[k ^ bit], one) for k, one in enumerate(blocks)]
        bit *= 2
    return jnp.concatenate(blocks, 1)


def erf_of(value):
    value = jnp.clip(value, -3.832506856900711, 3.832506856900711)
    square = value * value
    top = jnp.float32(0.00022905065861350646)
    for c in (
        0.0034082910107109506,
        0.050955695062380861,
        0.18520832239976145,
        1.128379143519084,
    ):
        top = top * square + c
    low = jnp.float32(-1.1791602954361697e-7)
    for c in (
        0.000023547966471313185,
        0.0010179625278914885,
        0.014070470171167667,
        0.11098505178285362,
        0.49746925110067538,
        1.0,
    ):
        low = low * square + c
    return value * top / low


def assemble(info, pieces, w_ref):
    half = w_ref.shape[1] // 2

    def place(slot, at, ref):
        rows = ref.shape[0]
        span = slice(slot * rows, (slot + 1) * rows)
        if len(pieces) == 1:
            mine = pl.multiple_of(info[1] * half, 128)
            other = pl.multiple_of((1 - info[1]) * half, 128)
            w_ref[span, :half] = ref[:, pl.ds(mine, half)]
            w_ref[span, half:] = ref[:, pl.ds(other, half)]
        else:
            target = info[1] if at == 0 else 1 - info[1]
            w_ref[span, pl.ds(pl.multiple_of(target * half, 128), half)] = ref[...]

    for at, (shard, ones, twos) in enumerate(pieces):
        place(0, at, shard)
        count = len(ones) + 1
        for k in range(1, count):
            pl.when(k <= info[0])(functools.partial(place, k, at, ones[k - 1]))
            if count - 1 - k < len(twos):
                pl.when(k > info[0])(functools.partial(place, k, at, twos[count - 1 - k]))


def flat_pieces(pieces):
    return [ref for shard, ones, twos in pieces for ref in (shard, *ones, *twos)]


def split_pieces(n, count, refs):
    size = 2 * n - 2
    groups = [refs[at * size : (at + 1) * size] for at in range(count)]
    return [(group[0], group[1:n], group[n:]) for group in groups], refs[count * size :]


ROWS = 104


def up_kernel(n, count, info, *refs):
    pieces, rest = split_pieces(n, count, refs)
    feats, w_ref, hidden_ref, send_ref, slope_ref, preact_ref = rest
    assemble(info, pieces, w_ref)
    half = send_ref.shape[1]
    for part in range(2):
        columns = slice(part * half, (part + 1) * half)
        preact_ref[...] = jnp.dot(
            feats[...], w_ref[:, columns], preferred_element_type=jnp.float32
        )

        def step(at, carry):
            rows = pl.ds(pl.multiple_of(at * ROWS, ROWS), ROWS)
            value = preact_ref[rows, :]
            cumulative = 0.5 * (1.0 + erf_of(value * reciprocal_root))
            density = normal_peak * jnp.exp(-0.5 * value * value)
            hidden = (value * cumulative).astype(jnp.bfloat16)
            hidden_ref[rows, columns] = hidden
            if part:
                send_ref[rows, :] = hidden
            slope_ref[rows, columns] = cumulative + value * density
            return carry

        lax.fori_loop(0, preact_ref.shape[0] // ROWS, step, 0)


def down_kernel(n, count, info, *refs):
    pieces, (cot, slope_ref, grad_ref, send_ref, w_ref) = split_pieces(n, count, refs)
    assemble(info, pieces, w_ref)
    half = send_ref.shape[1]
    for part in range(2):
        columns = slice(part * half, (part + 1) * half)
        hidden_grad = jnp.dot(cot[...], w_ref[:, columns], preferred_element_type=jnp.float32)
        grad = (hidden_grad * slope_ref[:, columns]).astype(jnp.bfloat16)
        grad_ref[:, columns] = grad
        if part:
            send_ref[...] = grad


LIMIT = pltpu.CompilerParams(vmem_limit_bytes=12 * 2**20)
VMEM = pl.BlockSpec(memory_space=pltpu.VMEM)
SMEM = pl.BlockSpec(memory_space=pltpu.SMEM)


def product_cost(m, k, n, moved):
    return pl.CostEstimate(flops=2 * m * k * n, bytes_accessed=moved, transcendentals=0)


def up_stage(info, pieces, feats, width):
    n, flat = len(pieces[0][1]) + 1, flat_pieces(pieces)
    depth, tokens = feats.shape[1], feats.shape[0]
    return pl.pallas_call(
        functools.partial(up_kernel, n, len(pieces)),
        out_shape=[
            jax.ShapeDtypeStruct((depth, width), jnp.bfloat16),
            jax.ShapeDtypeStruct((tokens, width), jnp.bfloat16),
            jax.ShapeDtypeStruct((tokens, width // 2), jnp.bfloat16),
            jax.ShapeDtypeStruct((tokens, width), jnp.float32),
        ],
        in_specs=[SMEM] + [VMEM] * (len(flat) + 1),
        out_specs=[VMEM] * 4,
        scratch_shapes=[pltpu.VMEM((tokens, width // 2), jnp.float32)],
        cost_estimate=product_cost(tokens, depth, 4 * width, 6 * depth * width),
        compiler_params=LIMIT,
        name="up_stage",
    )(info, *flat, feats)


def down_stage(info, pieces, cot, slope):
    n, flat = len(pieces[0][1]) + 1, flat_pieces(pieces)
    depth, width, tokens = cot.shape[1], slope.shape[1], cot.shape[0]
    return pl.pallas_call(
        functools.partial(down_kernel, n, len(pieces)),
        out_shape=[
            jax.ShapeDtypeStruct((tokens, width), jnp.bfloat16),
            jax.ShapeDtypeStruct((tokens, width // 2), jnp.bfloat16),
        ],
        in_specs=[SMEM] + [VMEM] * (len(flat) + 2),
        out_specs=[VMEM] * 2,
        scratch_shapes=[pltpu.VMEM((depth, width), jnp.bfloat16)],
        cost_estimate=product_cost(tokens, depth, 3 * width, 6 * depth * width),
        compiler_params=LIMIT,
        name="down_stage",
    )(info, *flat, cot, slope)


def coded(square):
    return (square * square).astype(jnp.bfloat16)


def decoded(code):
    return jnp.sqrt(code.astype(jnp.float32))


def sums_kernel(images, slot, n, left_own, left_other, right_own, right_other, *refs):
    grads, squares, (padded, total, total_square) = refs[:n], refs[n : 2 * n], refs[2 * n :]
    depth, width = padded.shape[1:]
    rows = grads[0].shape[0]
    for sample, right in enumerate((right_own, right_other)):
        for image in range(images):
            at = sample * images + image
            padded[at, :slot, :] = right[image * slot : (image + 1) * slot, :width]
            padded[at, slot:, :] = jnp.zeros((depth - slot, width), jnp.bfloat16)
    for k in range(n):
        span = slice(k * rows, (k + 1) * rows)
        for at in range(2 * images):
            left = left_own if at < images else left_other
            image = at % images
            one = jnp.dot(
                left[span, image * depth : (image + 1) * depth],
                padded[at],
                preferred_element_type=jnp.float32,
            )
            if at == 0:
                total[...] = one
                total_square[...] = one * one
            elif at < 2 * images - 1:
                total[...] += one
                total_square[...] += one * one
            else:
                grads[k][...] = total[...] + one
                square = total_square[...] + one * one
                squares[k][...] = coded(square) if k else square


def image_sums(left_own, left_other, right_own, right_other, images, slot, n):
    rows, width = left_own.shape[0] // n, right_other.shape[1]
    depth = left_own.shape[1] // images
    outs = [jax.ShapeDtypeStruct((rows, width), jnp.float32)] * (n + 1)
    outs += [jax.ShapeDtypeStruct((rows, width), jnp.bfloat16)] * (n - 1)
    found = pl.pallas_call(
        functools.partial(sums_kernel, images, slot, n),
        out_shape=outs,
        in_specs=[VMEM] * 4,
        out_specs=[VMEM] * len(outs),
        scratch_shapes=[
            pltpu.VMEM((2 * images, depth, width), jnp.bfloat16),
            pltpu.VMEM((rows, width), jnp.float32),
            pltpu.VMEM((rows, width), jnp.float32),
        ],
        cost_estimate=product_cost(n * rows, 4 * images * depth, width, 10 * n * rows * width),
        compiler_params=LIMIT,
        name="image_sums",
    )(left_own, left_other, right_own, right_other)
    return found[:n], found[n : n + 1], found[n + 1 :]


def scatter_line(sums, n):
    grads, squares, sends = sums
    me = lax.axis_index("dp")
    inner = (me > 0) & (me < n - 1)
    one, two = exchange_one(grads[n - 1]), None
    for stage in range(2, n):
        send_one = grads[n - stage]
        if two is not None:
            send_one = send_one + jnp.where(inner, two, 0)
        send_two = grads[stage] + one
        one, two = exchange_one(send_one), exchange_two(send_two)
    far = [swap_bit(sends[k - 1], "dp", k) for k in range(n - 1, 0, -1)]
    return (grads[0], one, two), (squares[0], *far)


def finish_kernel(count, samples, info, precision, grad, one, two, square, *refs):
    far, before, (new_ref, raw_ref, sum_ref) = refs[:3], refs[3:-3], refs[-3:]
    rows, half = grad.shape
    mine = pl.ds(pl.multiple_of(info[1] * half, 128), half)
    inner = info[2] > 0
    total = grad[...] + one[...] + jnp.where(inner, two[...], 0.0)
    squares = square[...]
    for ref in far:
        squares = squares + decoded(ref[...])
    new, raw = update(total, squares, precision[:, mine], samples, count)
    new_ref[...] = new
    raw_ref[...] = raw
    part = (raw * raw).reshape(rows // 8, 8, half).sum(0)
    part = sum(part[:, at : at + 128] for at in range(0, half, 128))
    part = jnp.sum(part, axis=0, keepdims=True)
    sum_ref[...] = part + before[0][...] if before else part


def finish(info, precision, grads, squares, before, samples, count):
    shape = grads[0].shape
    operands = (info, precision, *grads, *squares, *before)
    return pl.pallas_call(
        functools.partial(finish_kernel, count, samples),
        out_shape=[jax.ShapeDtypeStruct(shape, jnp.float32)] * 2
        + [jax.ShapeDtypeStruct((1, 128), jnp.float32)],
        in_specs=[SMEM] + [VMEM] * (len(operands) - 1),
        out_specs=[VMEM] * 3,
        compiler_params=LIMIT,
    )(*operands)


def step_kernel(entries, info, one, two, *refs):
    scale = step_scale(jnp.sum(one[...] + two[...]), entries)
    for (mean, raw, raw_other), out_ref in ((refs[:3], refs[6]), (refs[3:6], refs[7])):
        half = raw.shape[1]
        for core, part in ((info[1], raw), (1 - info[1], raw_other)):
            at = pl.ds(pl.multiple_of(core * half, 128), half)
            out_ref[:, at] = mean[:, at] - scale * part[...]


def mean_step(info, one, two, up, down, entries):
    return pl.pallas_call(
        functools.partial(step_kernel, entries),
        out_shape=[jax.ShapeDtypeStruct(up[0].shape, jnp.float32)] * 2,
        in_specs=[SMEM] + [VMEM] * 8,
        out_specs=[VMEM] * 2,
        compiler_params=LIMIT,
        name="mean_step",
    )(info, one, two, *up, *down)


def halves_kernel(info, grad, w_ref, near_ref, far_ref):
    rows = near_ref.shape[1] // 2
    for bit, out_ref in ((2, far_ref), (0, near_ref)):
        for j in range(2):
            at = pl.multiple_of((info[3] ^ bit ^ j) * rows, rows)
            out_ref[:, j * rows : (j + 1) * rows] = contract_cols(
                grad[...], w_ref[pl.ds(at, rows), :]
            )


def input_halves(info, grad, w_up):
    tokens, depth = grad.shape[0], w_up.shape[0]
    return pl.pallas_call(
        halves_kernel,
        out_shape=[jax.ShapeDtypeStruct((tokens, depth // 2), jnp.float32)] * 2,
        in_specs=[SMEM] + [VMEM] * 2,
        out_specs=[VMEM] * 2,
        compiler_params=LIMIT,
        name="ig_halves",
    )(info, grad, w_up)


def after(value, earlier):
    return lax.optimization_barrier((value, earlier))[0]


def pad_images(value, images, slot):
    value = value.reshape(images, PATCHES, value.shape[-1])
    return jnp.pad(value, ((0, 0), (0, slot - PATCHES), (0, 0))).reshape(images * slot, -1)


def quad_sum(value, axis):
    pairs = [(j * 2 + core, (j ^ (1 + core)) * 2 + core) for j in range(4) for core in range(2)]
    near = lax.ppermute(value, (axis, "mc"), pairs)
    far = swap_bit(value, axis, 3)
    return value + far + near, swap_core(near)


def all_sum(value):
    one, two = quad_sum(value + swap_core(value), "mp")
    return quad_sum(one + two, "dp")


def join_kernel(info, own, other, out_ref):
    half = own.shape[1]
    for core, part in ((info[1], own), (1 - info[1], other)):
        out_ref[:, pl.ds(pl.multiple_of(core * half, 128), half)] = part[...]


def join(info, own, other):
    return pl.pallas_call(
        join_kernel,
        out_shape=jax.ShapeDtypeStruct((own.shape[0], 2 * own.shape[1]), jnp.float32),
        in_specs=[SMEM] + [VMEM] * 2,
        out_specs=VMEM,
        compiler_params=LIMIT,
    )(info, own, other)


def rows_kernel(images, slot, one, two, out_ref):
    total = one[...] + two[...]
    for image in range(images):
        piece = total[image * slot : (image + 1) * slot].T
        out_ref[:, image * PATCHES : (image + 1) * PATCHES] = piece[:, :PATCHES].astype(
            out_ref.dtype
        )


def join_rows(one, two, images, slot):
    return pl.pallas_call(
        functools.partial(rows_kernel, images, slot),
        out_shape=jax.ShapeDtypeStruct((one.shape[1], images * PATCHES), jnp.bfloat16),
        in_specs=[VMEM] * 2,
        out_specs=VMEM,
        compiler_params=LIMIT,
        name="ig_join",
    )(one, two).T[None]


def shards_line(*args):
    return line_step(*args)


def line_step(
    features, out_cotangent, mean_up, precision_up, noise_up, mean_down, precision_down, noise_down
):
    n = lax.axis_size("dp")
    me, place, core = lax.axis_index("dp"), lax.axis_index("mp"), lax.axis_index("mc")
    images = features.shape[0] // PATCHES
    slot = SLOT
    rows, width = mean_up.shape
    half = width // 2
    reach = jnp.where(me & 1, me, n - 1 - me)
    inner = (me > 0) & (me < n - 1)
    info = jnp.stack([reach, core, inner, place ^ me]).astype(jnp.int32)

    def gather(shard, first=None):
        ones, twos = [], []
        for stage in range(1, n):
            from_one, from_two = (ones[-1], twos[-1]) if ones else (shard, shard)
            if stage == 2 and first is not None:
                from_one, from_two = after((from_one, from_two), first)
            ones.append(exchange_one(from_two))
            if stage < n - 1:
                twos.append(exchange_two(from_one))
        return shard, ones, twos

    feats_raw, cot_raw = slots(features, rows), slots(out_cotangent[0], rows)
    feats, cot = pad_images(feats_raw, images, slot), pad_images(cot_raw, images, slot)
    feats_left = pad_images(feats_raw, images, DEPTH).T
    cot_left = pad_images(cot_raw, images, DEPTH).T
    shard_up = sample_weights(mean_up, precision_up, noise_up[0])
    gathered_up = [gather(shard_up, (feats, cot, feats_left, cot_left))]
    later_mean = after(mean_down, shard_up)
    gathered_down = [
        gather(sample_weights(later_mean[:, at], precision_down[:, at], noise_down[0][:, at]))
        for at in (slice(0, half), slice(half, width))
    ]

    cot_left_other = swap_core(cot_left)

    w_up, hidden, hidden_send, slope = up_stage(info, gathered_up, feats, width)
    hidden_other = swap_core(hidden_send)
    sums_down = image_sums(cot_left, cot_left_other, hidden, hidden_other, images, slot, n)
    grads_down, squares_down = scatter_line(sums_down, n)

    preact_grad, grad_send = down_stage(info, gathered_down, cot, slope)
    grad_other = swap_core(grad_send)
    sums_up = image_sums(feats_left, feats_left, preact_grad, grad_other, images, slot, n)
    grads_up, squares_up = scatter_line(sums_up, n)

    near_half, far_half = input_halves(info, preact_grad, w_up)
    near_half = near_half + swap_bit(far_half, "mp", 2)
    near = swap_bit(near_half[:, rows:], "mp", 1)
    input_grad = join_rows(near_half[:, :rows], near, images, slot)

    samples = lax.axis_size("mc")
    images_all = images * n

    new_down, raw_down, part = finish(
        info, precision_down, grads_down, squares_down, (), samples, images_all
    )
    all_new_down = join(info, new_down, swap_core(new_down))
    raw_down_other = swap_core(raw_down)
    new_up, raw_up, part = finish(
        info, precision_up, grads_up, squares_up, (part,), samples, images_all
    )
    all_new_up = join(info, new_up, swap_core(new_up))
    one, two = all_sum(part)
    raw_up_other = swap_core(raw_up)
    entries = 2 * rows * width * n * lax.axis_size("mp")
    new_mean_up, new_mean_down = mean_step(
        info,
        one,
        two,
        (mean_up, raw_up, raw_up_other),
        (mean_down, raw_down, raw_down_other),
        entries,
    )
    return new_mean_up, all_new_up, new_mean_down, all_new_down, input_grad


def solution(mesh):
    in_specs = (
        P("dp", None),
        P("mc", "dp", None),
        P("dp", "mp"),
        P("dp", "mp"),
        P("mc", "dp", "mp"),
        P("dp", "mp"),
        P("dp", "mp"),
        P("mc", "dp", "mp"),
    )
    out_specs = (P("dp", "mp"), P("dp", "mp"), P("dp", "mp"), P("dp", "mp"), P("mc", "dp", "mp"))
    sizes = mesh.shape
    line = sizes["dp"] == 4 and sizes["mp"] == 4 and sizes["mc"] == 2
    body = shards_line if line else shards_general
    return jax.shard_map(body, mesh=mesh, in_specs=in_specs, out_specs=out_specs, check_vma=False)
```

```python
import functools
import jax
import jax.numpy as jnp
from jax import lax
from jax.experimental import pallas as pl
from jax.experimental.pallas import tpu as pltpu
from jax.sharding import PartitionSpec as P


PATCHES = 197
SLOT = 208
DEPTH = 256


reciprocal_root = 0.7071067811865476
normal_peak = 0.3989422804014327
tempering = 100.0
damping = 4.0
average_rate = 0.25
step_rate = 0.05
clip_level = 0.01


def gelu_parts(preact):
    cumulative = 0.5 * (1.0 + lax.erf(preact * reciprocal_root))
    density = normal_peak * jnp.exp(-0.5 * preact * preact)
    return (preact * cumulative, cumulative + preact * density)


def sample_weights(center, precision, noise_draw):
    spread = 1.0 / jnp.sqrt(tempering * (precision + damping))
    return (center + spread * noise_draw).astype(jnp.bfloat16)


def contract_rows(left, right):
    return lax.dot_general(
        left, right, (((0,), (0,)), ((), ())), preferred_element_type=jnp.float32
    )


def contract_cols(left, right):
    return lax.dot_general(
        left, right, (((1,), (1,)), ((), ())), preferred_element_type=jnp.float32
    )


def shards_general(
    features, out_cotangent, mean_up, precision_up, noise_up, mean_down, precision_down, noise_down
):
    w_up = lax.all_gather(sample_weights(mean_up, precision_up, noise_up[0]), "dp", axis=0, tiled=True)
    w_down = lax.all_gather(
        sample_weights(mean_down, precision_down, noise_down[0]), "dp", axis=0, tiled=True
    )
    cotangent = out_cotangent[0]
    preact = jnp.dot(features, w_up, preferred_element_type=jnp.float32)
    gelu_value, gelu_slope = gelu_parts(preact)
    hidden = gelu_value.astype(jnp.bfloat16)
    hidden_grad = jnp.dot(cotangent, w_down, preferred_element_type=jnp.float32)
    preact_grad = (hidden_grad * gelu_slope).astype(jnp.bfloat16)
    partial_value = contract_cols(preact_grad, w_up)
    input_grad = lax.psum_scatter(partial_value, "mp", scatter_dimension=1, tiled=True).astype(
        jnp.bfloat16
    )[None]
    images = features.shape[0] // PATCHES
    totals = [jnp.zeros(w_up.shape, jnp.float32)] * 4
    for image in range(images):
        rows = slice(image * PATCHES, (image + 1) * PATCHES)
        grad_up = contract_rows(features[rows], preact_grad[rows])
        grad_down = contract_rows(cotangent[rows], hidden[rows])
        terms = (grad_up, grad_up * grad_up, grad_down, grad_down * grad_down)
        totals = [total + term for total, term in zip(totals, terms)]
    totals = [lax.psum_scatter(t, "dp", scatter_dimension=0, tiled=True) for t in totals]
    totals = lax.psum(tuple(totals), "mc")
    samples = lax.axis_size("mc")
    images_all = images * lax.axis_size("dp")
    raws, news = [], []
    for (grad, square), precision in zip(
        (totals[:2], totals[2:]), (precision_up, precision_down)
    ):
        new, raw = update(grad, square, precision, samples, images_all)
        raws.append(raw)
        news.append(new)
    entries = 2 * raws[0].size * lax.axis_size("dp") * lax.axis_size("mp")
    local_sum = jnp.sum(raws[0] * raws[0]) + jnp.sum(raws[1] * raws[1])
    scale = step_scale(lax.psum(local_sum, ("dp", "mp")), entries)
    return (mean_up - scale * raws[0], news[0], mean_down - scale * raws[1], news[1], input_grad)


def precision_update(precision, square):
    return (1.0 - average_rate) * precision + average_rate * square


def update(grad_sum, square_sum, precision, samples, images_all):
    new = precision_update(precision, square_sum / (samples * images_all))
    return new, (grad_sum / samples) / (new + damping)


def step_scale(global_sum, entries):
    root_mean = jnp.sqrt(global_sum / entries)
    return step_rate * (1.0 / jnp.maximum(clip_level, root_mean))


def swap_core(value):
    return lax.ppermute(value, "mc", [(0, 1), (1, 0)])


def swap_bit(value, axis, bit):
    size = lax.axis_size(axis)
    return lax.ppermute(value, axis, [(j, j ^ bit) for j in range(size)])


def exchange_one(value):
    return swap_bit(value, "dp", 1)


def exchange_two(value):
    last, cores = lax.axis_size("dp") - 1, lax.axis_size("mc")
    pairs = []
    for j in range(last + 1):
        for core in range(cores):
            to = (j, 1 - core) if j in (0, last) else (((j - 1) ^ 1) + 1, core)
            pairs.append((j * cores + core, to[0] * cores + to[1]))
    return lax.ppermute(value, ("dp", "mc"), pairs)


def slots(value, size):
    me = lax.axis_index("dp")
    blocks = [value[:, k * size : (k + 1) * size] for k in range(lax.axis_size("dp"))]
    bit = 1
    while bit < len(blocks):
        blocks = [jnp.where(me & bit, blocks[k ^ bit], one) for k, one in enumerate(blocks)]
        bit *= 2
    return jnp.concatenate(blocks, 1)


def erf_of(value):
    value = jnp.clip(value, -3.832506856900711, 3.832506856900711)
    square = value * value
    top = jnp.float32(0.00022905065861350646)
    for c in (
        0.0034082910107109506,
        0.050955695062380861,
        0.18520832239976145,
        1.128379143519084,
    ):
        top = top * square + c
    low = jnp.float32(-1.1791602954361697e-7)
    for c in (
        0.000023547966471313185,
        0.0010179625278914885,
        0.014070470171167667,
        0.11098505178285362,
        0.49746925110067538,
        1.0,
    ):
        low = low * square + c
    return value * top / low


def assemble(info, pieces, w_ref):
    half = w_ref.shape[1] // 2

    def place(slot, at, ref):
        rows = ref.shape[0]
        span = slice(slot * rows, (slot + 1) * rows)
        if len(pieces) == 1:
            mine = pl.multiple_of(info[1] * half, 128)
            other = pl.multiple_of((1 - info[1]) * half, 128)
            w_ref[span, :half] = ref[:, pl.ds(mine, half)]
            w_ref[span, half:] = ref[:, pl.ds(other, half)]
        else:
            target = info[1] if at == 0 else 1 - info[1]
            w_ref[span, pl.ds(pl.multiple_of(target * half, 128), half)] = ref[...]

    for at, (shard, ones, twos) in enumerate(pieces):
        place(0, at, shard)
        count = len(ones) + 1
        for k in range(1, count):
            pl.when(k <= info[0])(functools.partial(place, k, at, ones[k - 1]))
            if count - 1 - k < len(twos):
                pl.when(k > info[0])(functools.partial(place, k, at, twos[count - 1 - k]))


def flat_pieces(pieces):
    return [ref for shard, ones, twos in pieces for ref in (shard, *ones, *twos)]


def split_pieces(n, count, refs):
    size = 2 * n - 2
    groups = [refs[at * size : (at + 1) * size] for at in range(count)]
    return [(group[0], group[1:n], group[n:]) for group in groups], refs[count * size :]


ROWS = 104


def up_kernel(n, count, info, *refs):
    pieces, rest = split_pieces(n, count, refs)
    feats, w_ref, hidden_ref, send_ref, slope_ref, preact_ref = rest
    assemble(info, pieces, w_ref)
    half = send_ref.shape[1]
    for part in range(2):
        columns = slice(part * half, (part + 1) * half)
        preact_ref[...] = jnp.dot(
            feats[...], w_ref[:, columns], preferred_element_type=jnp.float32
        )

        def step(at, carry):
            rows = pl.ds(pl.multiple_of(at * ROWS, ROWS), ROWS)
            value = preact_ref[rows, :]
            cumulative = 0.5 * (1.0 + erf_of(value * reciprocal_root))
            density = normal_peak * jnp.exp(-0.5 * value * value)
            hidden = (value * cumulative).astype(jnp.bfloat16)
            hidden_ref[rows, columns] = hidden
            if part:
                send_ref[rows, :] = hidden
            slope_ref[rows, columns] = cumulative + value * density
            return carry

        lax.fori_loop(0, preact_ref.shape[0] // ROWS, step, 0)


def down_kernel(n, count, info, *refs):
    pieces, (cot, slope_ref, grad_ref, send_ref, w_ref) = split_pieces(n, count, refs)
    assemble(info, pieces, w_ref)
    half = send_ref.shape[1]
    for part in range(2):
        columns = slice(part * half, (part + 1) * half)
        hidden_grad = jnp.dot(cot[...], w_ref[:, columns], preferred_element_type=jnp.float32)
        grad = (hidden_grad * slope_ref[:, columns]).astype(jnp.bfloat16)
        grad_ref[:, columns] = grad
        if part:
            send_ref[...] = grad


LIMIT = pltpu.CompilerParams(vmem_limit_bytes=12 * 2**20)
VMEM = pl.BlockSpec(memory_space=pltpu.VMEM)
SMEM = pl.BlockSpec(memory_space=pltpu.SMEM)


def product_cost(m, k, n, moved):
    return pl.CostEstimate(flops=2 * m * k * n, bytes_accessed=moved, transcendentals=0)


def up_stage(info, pieces, feats, width):
    n, flat = len(pieces[0][1]) + 1, flat_pieces(pieces)
    depth, tokens = feats.shape[1], feats.shape[0]
    return pl.pallas_call(
        functools.partial(up_kernel, n, len(pieces)),
        out_shape=[
            jax.ShapeDtypeStruct((depth, width), jnp.bfloat16),
            jax.ShapeDtypeStruct((tokens, width), jnp.bfloat16),
            jax.ShapeDtypeStruct((tokens, width // 2), jnp.bfloat16),
            jax.ShapeDtypeStruct((tokens, width), jnp.float32),
        ],
        in_specs=[SMEM] + [VMEM] * (len(flat) + 1),
        out_specs=[VMEM] * 4,
        scratch_shapes=[pltpu.VMEM((tokens, width // 2), jnp.float32)],
        cost_estimate=product_cost(tokens, depth, 4 * width, 6 * depth * width),
        compiler_params=LIMIT,
        name="up_stage",
    )(info, *flat, feats)


def down_stage(info, pieces, cot, slope):
    n, flat = len(pieces[0][1]) + 1, flat_pieces(pieces)
    depth, width, tokens = cot.shape[1], slope.shape[1], cot.shape[0]
    return pl.pallas_call(
        functools.partial(down_kernel, n, len(pieces)),
        out_shape=[
            jax.ShapeDtypeStruct((tokens, width), jnp.bfloat16),
            jax.ShapeDtypeStruct((tokens, width // 2), jnp.bfloat16),
        ],
        in_specs=[SMEM] + [VMEM] * (len(flat) + 2),
        out_specs=[VMEM] * 2,
        scratch_shapes=[pltpu.VMEM((depth, width), jnp.bfloat16)],
        cost_estimate=product_cost(tokens, depth, 3 * width, 6 * depth * width),
        compiler_params=LIMIT,
        name="down_stage",
    )(info, *flat, cot, slope)


def coded(square):
    return (square * square).astype(jnp.bfloat16)


def decoded(code):
    return jnp.sqrt(code.astype(jnp.float32))


CODE_SCALE = 128.0


def grad_coded(grad):
    scaled = grad * CODE_SCALE
    return (scaled * jnp.abs(scaled) * (scaled * scaled)).astype(jnp.bfloat16)


def grad_decoded(code):
    code = code.astype(jnp.float32)
    root = jnp.sqrt(jnp.sqrt(jnp.abs(code))) * (1.0 / CODE_SCALE)
    return jnp.where(code < 0, -root, root)


def sums_kernel(images, slot, n, left_own, left_other, right_own, right_other, *refs):
    grads, squares, codes, (padded, total, total_square) = (
        refs[:n], refs[n : 2 * n], refs[2 * n : 2 * n + 2], refs[2 * n + 2 :]
    )
    depth, width = padded.shape[1:]
    rows = grads[0].shape[0]
    for sample, right in enumerate((right_own, right_other)):
        for image in range(images):
            at = sample * images + image
            padded[at, :slot, :] = right[image * slot : (image + 1) * slot, :width]
            padded[at, slot:, :] = jnp.zeros((depth - slot, width), jnp.bfloat16)
    for k in range(n):
        span = slice(k * rows, (k + 1) * rows)
        for at in range(2 * images):
            left = left_own if at < images else left_other
            image = at % images
            one = jnp.dot(
                left[span, image * depth : (image + 1) * depth],
                padded[at],
                preferred_element_type=jnp.float32,
            )
            if at == 0:
                total[...] = one
                total_square[...] = one * one
            elif at < 2 * images - 1:
                total[...] += one
                total_square[...] += one * one
            else:
                grad = total[...] + one
                grads[k][...] = grad
                if k >= n - 2:
                    codes[k - n + 2][...] = grad_coded(grad)
                square = total_square[...] + one * one
                squares[k][...] = coded(square) if k else square


def image_sums(left_own, left_other, right_own, right_other, images, slot, n):
    rows, width = left_own.shape[0] // n, right_other.shape[1]
    depth = left_own.shape[1] // images
    outs = [jax.ShapeDtypeStruct((rows, width), jnp.float32)] * (n + 1)
    outs += [jax.ShapeDtypeStruct((rows, width), jnp.bfloat16)] * (n + 1)
    found = pl.pallas_call(
        functools.partial(sums_kernel, images, slot, n),
        out_shape=outs,
        in_specs=[VMEM] * 4,
        out_specs=[VMEM] * len(outs),
        scratch_shapes=[
            pltpu.VMEM((2 * images, depth, width), jnp.bfloat16),
            pltpu.VMEM((rows, width), jnp.float32),
            pltpu.VMEM((rows, width), jnp.float32),
        ],
        cost_estimate=product_cost(n * rows, 4 * images * depth, width, 10 * n * rows * width),
        compiler_params=LIMIT,
        name="image_sums",
    )(left_own, left_other, right_own, right_other)
    return found[:n], found[n], found[n + 1 : 2 * n], found[2 * n :]


def scatter_line(sums, n):
    grads, square, sends, codes = sums
    me = lax.axis_index("dp")
    inner = (me > 0) & (me < n - 1)
    one, two = exchange_one(codes[1]), None
    for stage in range(2, n):
        if two is None:
            send_one = codes[0]
        else:
            send_one = grad_coded(grads[n - stage] + jnp.where(inner, grad_decoded(two), 0))
        send_two = grad_coded(grads[stage] + grad_decoded(one))
        one, two = exchange_one(send_one), exchange_two(send_two)
    far = [swap_bit(sends[k - 1], "dp", k) for k in range(n - 1, 0, -1)]
    return (grads[0], one, two), (square, *far)


def finish_kernel(count, samples, info, precision, grad, one, two, square, *refs):
    far, before, (new_ref, raw_ref, sum_ref) = refs[:3], refs[3:-3], refs[-3:]
    rows, half = grad.shape
    mine = pl.ds(pl.multiple_of(info[1] * half, 128), half)
    inner = info[2] > 0
    total = grad[...] + grad_decoded(one[...]) + jnp.where(inner, grad_decoded(two[...]), 0.0)
    squares = square[...]
    for ref in far:
        squares = squares + decoded(ref[...])
    new, raw = update(total, squares, precision[:, mine], samples, count)
    new_ref[...] = new
    raw_ref[...] = raw
    part = (raw * raw).reshape(rows // 8, 8, half).sum(0)
    part = sum(part[:, at : at + 128] for at in range(0, half, 128))
    part = jnp.sum(part, axis=0, keepdims=True)
    sum_ref[...] = part + before[0][...] if before else part


def finish(info, precision, grads, squares, before, samples, count):
    shape = grads[0].shape
    operands = (info, precision, *grads, *squares, *before)
    return pl.pallas_call(
        functools.partial(finish_kernel, count, samples),
        out_shape=[jax.ShapeDtypeStruct(shape, jnp.float32)] * 2
        + [jax.ShapeDtypeStruct((1, 128), jnp.float32)],
        in_specs=[SMEM] + [VMEM] * (len(operands) - 1),
        out_specs=[VMEM] * 3,
        compiler_params=LIMIT,
    )(*operands)


def step_kernel(entries, info, one, two, *refs):
    scale = step_scale(jnp.sum(one[...] + two[...]), entries)
    for (mean, raw, raw_other), out_ref in ((refs[:3], refs[6]), (refs[3:6], refs[7])):
        half = raw.shape[1]
        for core, part in ((info[1], raw), (1 - info[1], raw_other)):
            at = pl.ds(pl.multiple_of(core * half, 128), half)
            out_ref[:, at] = mean[:, at] - scale * part[...]


def mean_step(info, one, two, up, down, entries):
    return pl.pallas_call(
        functools.partial(step_kernel, entries),
        out_shape=[jax.ShapeDtypeStruct(up[0].shape, jnp.float32)] * 2,
        in_specs=[SMEM] + [VMEM] * 8,
        out_specs=[VMEM] * 2,
        compiler_params=LIMIT,
        name="mean_step",
    )(info, one, two, *up, *down)


def halves_kernel(info, grad, w_ref, near_ref, far_ref):
    rows = near_ref.shape[1] // 2
    for bit, out_ref in ((2, far_ref), (0, near_ref)):
        for j in range(2):
            at = pl.multiple_of((info[3] ^ bit ^ j) * rows, rows)
            out_ref[:, j * rows : (j + 1) * rows] = contract_cols(
                grad[...], w_ref[pl.ds(at, rows), :]
            )


def input_halves(info, grad, w_up):
    tokens, depth = grad.shape[0], w_up.shape[0]
    return pl.pallas_call(
        halves_kernel,
        out_shape=[jax.ShapeDtypeStruct((tokens, depth // 2), jnp.float32)] * 2,
        in_specs=[SMEM] + [VMEM] * 2,
        out_specs=[VMEM] * 2,
        compiler_params=LIMIT,
        name="ig_halves",
    )(info, grad, w_up)


def after(value, earlier):
    return lax.optimization_barrier((value, earlier))[0]


def pad_images(value, images, slot):
    value = value.reshape(images, PATCHES, value.shape[-1])
    return jnp.pad(value, ((0, 0), (0, slot - PATCHES), (0, 0))).reshape(images * slot, -1)


def quad_sum(value, axis):
    pairs = [(j * 2 + core, (j ^ (1 + core)) * 2 + core) for j in range(4) for core in range(2)]
    near = lax.ppermute(value, (axis, "mc"), pairs)
    far = swap_bit(value, axis, 3)
    return value + far + near, swap_core(near)


def all_sum(value):
    one, two = quad_sum(value + swap_core(value), "mp")
    return quad_sum(one + two, "dp")


def join_kernel(info, own, other, out_ref):
    half = own.shape[1]
    for core, part in ((info[1], own), (1 - info[1], other)):
        out_ref[:, pl.ds(pl.multiple_of(core * half, 128), half)] = part[...]


def join(info, own, other):
    return pl.pallas_call(
        join_kernel,
        out_shape=jax.ShapeDtypeStruct((own.shape[0], 2 * own.shape[1]), jnp.float32),
        in_specs=[SMEM] + [VMEM] * 2,
        out_specs=VMEM,
        compiler_params=LIMIT,
    )(info, own, other)


def rows_kernel(images, slot, one, two, out_ref):
    total = one[...] + two[...]
    for image in range(images):
        piece = total[image * slot : (image + 1) * slot].T
        out_ref[:, image * PATCHES : (image + 1) * PATCHES] = piece[:, :PATCHES].astype(
            out_ref.dtype
        )


def join_rows(one, two, images, slot):
    return pl.pallas_call(
        functools.partial(rows_kernel, images, slot),
        out_shape=jax.ShapeDtypeStruct((one.shape[1], images * PATCHES), jnp.bfloat16),
        in_specs=[VMEM] * 2,
        out_specs=VMEM,
        compiler_params=LIMIT,
        name="ig_join",
    )(one, two).T[None]


def shards_line(*args):
    return line_step(*args)


def line_step(
    features, out_cotangent, mean_up, precision_up, noise_up, mean_down, precision_down, noise_down
):
    n = lax.axis_size("dp")
    me, place, core = lax.axis_index("dp"), lax.axis_index("mp"), lax.axis_index("mc")
    images = features.shape[0] // PATCHES
    slot = SLOT
    rows, width = mean_up.shape
    half = width // 2
    reach = jnp.where(me & 1, me, n - 1 - me)
    inner = (me > 0) & (me < n - 1)
    info = jnp.stack([reach, core, inner, place ^ me]).astype(jnp.int32)

    def gather(shard, first=None):
        ones, twos = [], []
        for stage in range(1, n):
            from_one, from_two = (ones[-1], twos[-1]) if ones else (shard, shard)
            if stage == 2 and first is not None:
                from_one, from_two = after((from_one, from_two), first)
            ones.append(exchange_one(from_two))
            if stage < n - 1:
                twos.append(exchange_two(from_one))
        return shard, ones, twos

    feats_raw, cot_raw = slots(features, rows), slots(out_cotangent[0], rows)
    feats, cot = pad_images(feats_raw, images, slot), pad_images(cot_raw, images, slot)
    feats_left = pad_images(feats_raw, images, DEPTH).T
    cot_left = pad_images(cot_raw, images, DEPTH).T
    shard_up = sample_weights(mean_up, precision_up, noise_up[0])
    gathered_up = [gather(shard_up, (feats, cot, feats_left, cot_left))]
    later_mean = after(mean_down, shard_up)
    gathered_down = [
        gather(sample_weights(later_mean[:, at], precision_down[:, at], noise_down[0][:, at]))
        for at in (slice(0, half), slice(half, width))
    ]

    cot_left_other = swap_core(cot_left)

    w_up, hidden, hidden_send, slope = up_stage(info, gathered_up, feats, width)
    hidden_other = swap_core(hidden_send)
    sums_down = image_sums(cot_left, cot_left_other, hidden, hidden_other, images, slot, n)
    grads_down, squares_down = scatter_line(sums_down, n)

    preact_grad, grad_send = down_stage(info, gathered_down, cot, slope)
    grad_other = swap_core(grad_send)
    sums_up = image_sums(feats_left, feats_left, preact_grad, grad_other, images, slot, n)
    grads_up, squares_up = scatter_line(sums_up, n)

    near_half, far_half = input_halves(info, preact_grad, w_up)
    near_half = near_half + swap_bit(far_half, "mp", 2)
    near = swap_bit(near_half[:, rows:], "mp", 1)
    input_grad = join_rows(near_half[:, :rows], near, images, slot)

    samples = lax.axis_size("mc")
    images_all = images * n

    new_down, raw_down, part = finish(
        info, precision_down, grads_down, squares_down, (), samples, images_all
    )
    all_new_down = join(info, new_down, swap_core(new_down))
    raw_down_other = swap_core(raw_down)
    new_up, raw_up, part = finish(
        info, precision_up, grads_up, squares_up, (part,), samples, images_all
    )
    all_new_up = join(info, new_up, swap_core(new_up))
    one, two = all_sum(part)
    raw_up_other = swap_core(raw_up)
    entries = 2 * rows * width * n * lax.axis_size("mp")
    new_mean_up, new_mean_down = mean_step(
        info,
        one,
        two,
        (mean_up, raw_up, raw_up_other),
        (mean_down, raw_down, raw_down_other),
        entries,
    )
    return new_mean_up, all_new_up, new_mean_down, all_new_down, input_grad


def solution(mesh):
    in_specs = (
        P("dp", None),
        P("mc", "dp", None),
        P("dp", "mp"),
        P("dp", "mp"),
        P("mc", "dp", "mp"),
        P("dp", "mp"),
        P("dp", "mp"),
        P("mc", "dp", "mp"),
    )
    out_specs = (P("dp", "mp"), P("dp", "mp"), P("dp", "mp"), P("dp", "mp"), P("mc", "dp", "mp"))
    sizes = mesh.shape
    line = sizes["dp"] == 4 and sizes["mp"] == 4 and sizes["mc"] == 2
    body = shards_line if line else shards_general
    return jax.shard_map(body, mesh=mesh, in_specs=in_specs, out_specs=out_specs, check_vma=False)
```

```python
import functools
import jax
import jax.numpy as jnp
from jax import lax
from jax.experimental import pallas as pl
from jax.experimental.pallas import tpu as pltpu
from jax.sharding import PartitionSpec as P


PATCHES = 197
SLOT = 208
DEPTH = 256


reciprocal_root = 0.7071067811865476
normal_peak = 0.3989422804014327
tempering = 100.0
damping = 4.0
average_rate = 0.25
step_rate = 0.05
clip_level = 0.01


def gelu_parts(preact):
    cumulative = 0.5 * (1.0 + lax.erf(preact * reciprocal_root))
    density = normal_peak * jnp.exp(-0.5 * preact * preact)
    return (preact * cumulative, cumulative + preact * density)


def sample_weights(center, precision, noise_draw):
    spread = 1.0 / jnp.sqrt(tempering * (precision + damping))
    return (center + spread * noise_draw).astype(jnp.bfloat16)


def contract_rows(left, right):
    return lax.dot_general(
        left, right, (((0,), (0,)), ((), ())), preferred_element_type=jnp.float32
    )


def contract_cols(left, right):
    return lax.dot_general(
        left, right, (((1,), (1,)), ((), ())), preferred_element_type=jnp.float32
    )


def shards_general(
    features, out_cotangent, mean_up, precision_up, noise_up, mean_down, precision_down, noise_down
):
    w_up = lax.all_gather(sample_weights(mean_up, precision_up, noise_up[0]), "dp", axis=0, tiled=True)
    w_down = lax.all_gather(
        sample_weights(mean_down, precision_down, noise_down[0]), "dp", axis=0, tiled=True
    )
    cotangent = out_cotangent[0]
    preact = jnp.dot(features, w_up, preferred_element_type=jnp.float32)
    gelu_value, gelu_slope = gelu_parts(preact)
    hidden = gelu_value.astype(jnp.bfloat16)
    hidden_grad = jnp.dot(cotangent, w_down, preferred_element_type=jnp.float32)
    preact_grad = (hidden_grad * gelu_slope).astype(jnp.bfloat16)
    partial_value = contract_cols(preact_grad, w_up)
    input_grad = lax.psum_scatter(partial_value, "mp", scatter_dimension=1, tiled=True).astype(
        jnp.bfloat16
    )[None]
    images = features.shape[0] // PATCHES
    totals = [jnp.zeros(w_up.shape, jnp.float32)] * 4
    for image in range(images):
        rows = slice(image * PATCHES, (image + 1) * PATCHES)
        grad_up = contract_rows(features[rows], preact_grad[rows])
        grad_down = contract_rows(cotangent[rows], hidden[rows])
        terms = (grad_up, grad_up * grad_up, grad_down, grad_down * grad_down)
        totals = [total + term for total, term in zip(totals, terms)]
    totals = [lax.psum_scatter(t, "dp", scatter_dimension=0, tiled=True) for t in totals]
    totals = lax.psum(tuple(totals), "mc")
    samples = lax.axis_size("mc")
    images_all = images * lax.axis_size("dp")
    raws, news = [], []
    for (grad, square), precision in zip(
        (totals[:2], totals[2:]), (precision_up, precision_down)
    ):
        new, raw = update(grad, square, precision, samples, images_all)
        raws.append(raw)
        news.append(new)
    entries = 2 * raws[0].size * lax.axis_size("dp") * lax.axis_size("mp")
    local_sum = jnp.sum(raws[0] * raws[0]) + jnp.sum(raws[1] * raws[1])
    scale = step_scale(lax.psum(local_sum, ("dp", "mp")), entries)
    return (mean_up - scale * raws[0], news[0], mean_down - scale * raws[1], news[1], input_grad)


def precision_update(precision, square):
    return (1.0 - average_rate) * precision + average_rate * square


def update(grad_sum, square_sum, precision, samples, images_all):
    new = precision_update(precision, square_sum / (samples * images_all))
    return new, (grad_sum / samples) / (new + damping)


def step_scale(global_sum, entries):
    root_mean = jnp.sqrt(global_sum / entries)
    return step_rate * (1.0 / jnp.maximum(clip_level, root_mean))


def swap_core(value):
    return lax.ppermute(value, "mc", [(0, 1), (1, 0)])


def swap_bit(value, axis, bit):
    size = lax.axis_size(axis)
    return lax.ppermute(value, axis, [(j, j ^ bit) for j in range(size)])


def exchange_one(value):
    return swap_bit(value, "dp", 1)


def exchange_two(value):
    last, cores = lax.axis_size("dp") - 1, lax.axis_size("mc")
    pairs = []
    for j in range(last + 1):
        for core in range(cores):
            to = (j, 1 - core) if j in (0, last) else (((j - 1) ^ 1) + 1, core)
            pairs.append((j * cores + core, to[0] * cores + to[1]))
    return lax.ppermute(value, ("dp", "mc"), pairs)


def slots(value, size):
    me = lax.axis_index("dp")
    blocks = [value[:, k * size : (k + 1) * size] for k in range(lax.axis_size("dp"))]
    bit = 1
    while bit < len(blocks):
        blocks = [jnp.where(me & bit, blocks[k ^ bit], one) for k, one in enumerate(blocks)]
        bit *= 2
    return jnp.concatenate(blocks, 1)


def erf_of(value):
    value = jnp.clip(value, -3.832506856900711, 3.832506856900711)
    square = value * value
    top = jnp.float32(0.00022905065861350646)
    for c in (
        0.0034082910107109506,
        0.050955695062380861,
        0.18520832239976145,
        1.128379143519084,
    ):
        top = top * square + c
    low = jnp.float32(-1.1791602954361697e-7)
    for c in (
        0.000023547966471313185,
        0.0010179625278914885,
        0.014070470171167667,
        0.11098505178285362,
        0.49746925110067538,
        1.0,
    ):
        low = low * square + c
    return value * top / low


def assemble(info, pieces, w_ref):
    half = w_ref.shape[1] // 2

    def place(slot, at, ref):
        rows = ref.shape[0]
        span = slice(slot * rows, (slot + 1) * rows)
        if len(pieces) == 1:
            mine = pl.multiple_of(info[1] * half, 128)
            other = pl.multiple_of((1 - info[1]) * half, 128)
            w_ref[span, :half] = ref[:, pl.ds(mine, half)]
            w_ref[span, half:] = ref[:, pl.ds(other, half)]
        else:
            target = info[1] if at == 0 else 1 - info[1]
            w_ref[span, pl.ds(pl.multiple_of(target * half, 128), half)] = ref[...]

    for at, (shard, ones, twos) in enumerate(pieces):
        place(0, at, shard)
        count = len(ones) + 1
        for k in range(1, count):
            pl.when(k <= info[0])(functools.partial(place, k, at, ones[k - 1]))
            if count - 1 - k < len(twos):
                pl.when(k > info[0])(functools.partial(place, k, at, twos[count - 1 - k]))


def flat_pieces(pieces):
    return [ref for shard, ones, twos in pieces for ref in (shard, *ones, *twos)]


def split_pieces(n, count, refs):
    size = 2 * n - 2
    groups = [refs[at * size : (at + 1) * size] for at in range(count)]
    return [(group[0], group[1:n], group[n:]) for group in groups], refs[count * size :]


ROWS = 104


def up_kernel(n, count, info, *refs):
    pieces, rest = split_pieces(n, count, refs)
    feats, w_ref, hidden_ref, send_ref, slope_ref, preact_ref = rest
    assemble(info, pieces, w_ref)
    half = send_ref.shape[1]
    for part in range(2):
        columns = slice(part * half, (part + 1) * half)
        preact_ref[...] = jnp.dot(
            feats[...], w_ref[:, columns], preferred_element_type=jnp.float32
        )

        def step(at, carry):
            rows = pl.ds(pl.multiple_of(at * ROWS, ROWS), ROWS)
            value = preact_ref[rows, :]
            cumulative = 0.5 * (1.0 + erf_of(value * reciprocal_root))
            density = normal_peak * jnp.exp(-0.5 * value * value)
            hidden = (value * cumulative).astype(jnp.bfloat16)
            hidden_ref[rows, columns] = hidden
            if part:
                send_ref[rows, :] = hidden
            slope_ref[rows, columns] = cumulative + value * density
            return carry

        lax.fori_loop(0, preact_ref.shape[0] // ROWS, step, 0)


def down_kernel(n, count, info, *refs):
    pieces, (cot, slope_ref, grad_ref, send_ref, w_ref) = split_pieces(n, count, refs)
    assemble(info, pieces, w_ref)
    half = send_ref.shape[1]
    for part in range(2):
        columns = slice(part * half, (part + 1) * half)
        hidden_grad = jnp.dot(cot[...], w_ref[:, columns], preferred_element_type=jnp.float32)
        grad = (hidden_grad * slope_ref[:, columns]).astype(jnp.bfloat16)
        grad_ref[:, columns] = grad
        if part:
            send_ref[...] = grad


LIMIT = pltpu.CompilerParams(vmem_limit_bytes=12 * 2**20)
VMEM = pl.BlockSpec(memory_space=pltpu.VMEM)
SMEM = pl.BlockSpec(memory_space=pltpu.SMEM)


def product_cost(m, k, n, moved):
    return pl.CostEstimate(flops=2 * m * k * n, bytes_accessed=moved, transcendentals=0)


def up_stage(info, pieces, feats, width):
    n, flat = len(pieces[0][1]) + 1, flat_pieces(pieces)
    depth, tokens = feats.shape[1], feats.shape[0]
    return pl.pallas_call(
        functools.partial(up_kernel, n, len(pieces)),
        out_shape=[
            jax.ShapeDtypeStruct((depth, width), jnp.bfloat16),
            jax.ShapeDtypeStruct((tokens, width), jnp.bfloat16),
            jax.ShapeDtypeStruct((tokens, width // 2), jnp.bfloat16),
            jax.ShapeDtypeStruct((tokens, width), jnp.float32),
        ],
        in_specs=[SMEM] + [VMEM] * (len(flat) + 1),
        out_specs=[VMEM] * 4,
        scratch_shapes=[pltpu.VMEM((tokens, width // 2), jnp.float32)],
        cost_estimate=product_cost(tokens, depth, 4 * width, 6 * depth * width),
        compiler_params=LIMIT,
        name="up_stage",
    )(info, *flat, feats)


def down_stage(info, pieces, cot, slope):
    n, flat = len(pieces[0][1]) + 1, flat_pieces(pieces)
    depth, width, tokens = cot.shape[1], slope.shape[1], cot.shape[0]
    return pl.pallas_call(
        functools.partial(down_kernel, n, len(pieces)),
        out_shape=[
            jax.ShapeDtypeStruct((tokens, width), jnp.bfloat16),
            jax.ShapeDtypeStruct((tokens, width // 2), jnp.bfloat16),
        ],
        in_specs=[SMEM] + [VMEM] * (len(flat) + 2),
        out_specs=[VMEM] * 2,
        scratch_shapes=[pltpu.VMEM((depth, width), jnp.bfloat16)],
        cost_estimate=product_cost(tokens, depth, 3 * width, 6 * depth * width),
        compiler_params=LIMIT,
        name="down_stage",
    )(info, *flat, cot, slope)


GRAD_SCALE = 128.0
SQUARE_SCALE = 2.0**-16


def coded(value, scale):
    scaled = value * scale
    return (scaled * jnp.abs(scaled) * (scaled * scaled)).astype(jnp.bfloat16)


def decoded(code, scale):
    code = code.astype(jnp.float32)
    root = jnp.sqrt(jnp.sqrt(jnp.abs(code))) * (1.0 / scale)
    return jnp.where(code < 0, -root, root)


def store_pair(ref, grad, square):
    ref[0] = coded(grad, GRAD_SCALE)
    ref[1] = coded(square, SQUARE_SCALE)


def load_pair(ref):
    return decoded(ref[0], GRAD_SCALE), decoded(ref[1], SQUARE_SCALE)


def sums_kernel(images, slot, n, left_own, left_other, right_own, right_other, *refs):
    grads, squares, codes, (padded, total, total_square) = (
        refs[:n], refs[n : 2 * n], refs[2 * n : 2 * n + 2], refs[2 * n + 2 :]
    )
    depth, width = padded.shape[1:]
    rows = grads[0].shape[0]
    for sample, right in enumerate((right_own, right_other)):
        for image in range(images):
            at = sample * images + image
            padded[at, :slot, :] = right[image * slot : (image + 1) * slot, :width]
            padded[at, slot:, :] = jnp.zeros((depth - slot, width), jnp.bfloat16)
    for k in range(n):
        span = slice(k * rows, (k + 1) * rows)
        for at in range(2 * images):
            left = left_own if at < images else left_other
            image = at % images
            one = jnp.dot(
                left[span, image * depth : (image + 1) * depth],
                padded[at],
                preferred_element_type=jnp.float32,
            )
            if at == 0:
                total[...] = one
                total_square[...] = one * one
            elif at < 2 * images - 1:
                total[...] += one
                total_square[...] += one * one
            else:
                grad = total[...] + one
                grads[k][...] = grad
                square = total_square[...] + one * one
                squares[k][...] = square
                if k >= n - 2:
                    store_pair(codes[k - n + 2], grad, square)


def image_sums(left_own, left_other, right_own, right_other, images, slot, n):
    rows, width = left_own.shape[0] // n, right_other.shape[1]
    depth = left_own.shape[1] // images
    outs = [jax.ShapeDtypeStruct((rows, width), jnp.float32)] * (2 * n)
    outs += [jax.ShapeDtypeStruct((2, rows, width), jnp.bfloat16)] * 2
    found = pl.pallas_call(
        functools.partial(sums_kernel, images, slot, n),
        out_shape=outs,
        in_specs=[VMEM] * 4,
        out_specs=[VMEM] * len(outs),
        scratch_shapes=[
            pltpu.VMEM((2 * images, depth, width), jnp.bfloat16),
            pltpu.VMEM((rows, width), jnp.float32),
            pltpu.VMEM((rows, width), jnp.float32),
        ],
        cost_estimate=product_cost(n * rows, 4 * images * depth, width, 10 * n * rows * width),
        compiler_params=LIMIT,
        name="image_sums",
    )(left_own, left_other, right_own, right_other)
    return found[:n], found[n : 2 * n], found[2 * n :]


def hop_kernel(masked, info, grad, square, pair, out_ref):
    more, more_square = load_pair(pair)
    if masked:
        inner = info[2] > 0
        more, more_square = jnp.where(inner, more, 0.0), jnp.where(inner, more_square, 0.0)
    store_pair(out_ref, grad[...] + more, square[...] + more_square)


def hop(info, grad, square, pair, masked):
    return pl.pallas_call(
        functools.partial(hop_kernel, masked),
        out_shape=jax.ShapeDtypeStruct(pair.shape, pair.dtype),
        in_specs=[SMEM] + [VMEM] * 3,
        out_specs=VMEM,
        compiler_params=LIMIT,
        name="hop",
    )(info, grad, square, pair)


def scatter_line(info, sums, n):
    grads, squares, codes = sums
    one, two = exchange_one(codes[1]), None
    for stage in range(2, n):
        if two is None:
            send_one = codes[0]
        else:
            send_one = hop(info, grads[n - stage], squares[n - stage], two, True)
        send_two = hop(info, grads[stage], squares[stage], one, False)
        one, two = exchange_one(send_one), exchange_two(send_two)
    return grads[0], squares[0], one, two


def finish_kernel(count, samples, info, precision, grad, square, one, two, *refs):
    before, (new_ref, raw_ref, sum_ref) = refs[:-3], refs[-3:]
    rows, half = grad.shape
    mine = pl.ds(pl.multiple_of(info[1] * half, 128), half)
    inner = info[2] > 0
    grad_one, square_one = load_pair(one)
    grad_two, square_two = load_pair(two)
    total = grad[...] + grad_one + jnp.where(inner, grad_two, 0.0)
    squares = square[...] + square_one + jnp.where(inner, square_two, 0.0)
    new, raw = update(total, squares, precision[:, mine], samples, count)
    new_ref[...] = new
    raw_ref[...] = raw
    part = (raw * raw).reshape(rows // 8, 8, half).sum(0)
    part = sum(part[:, at : at + 128] for at in range(0, half, 128))
    part = jnp.sum(part, axis=0, keepdims=True)
    sum_ref[...] = part + before[0][...] if before else part


def finish(info, precision, sums, before, samples, count):
    shape = sums[0].shape
    operands = (info, precision, *sums, *before)
    return pl.pallas_call(
        functools.partial(finish_kernel, count, samples),
        out_shape=[jax.ShapeDtypeStruct(shape, jnp.float32)] * 2
        + [jax.ShapeDtypeStruct((1, 128), jnp.float32)],
        in_specs=[SMEM] + [VMEM] * (len(operands) - 1),
        out_specs=[VMEM] * 3,
        compiler_params=LIMIT,
    )(*operands)


def step_kernel(entries, info, one, two, *refs):
    scale = step_scale(jnp.sum(one[...] + two[...]), entries)
    for (mean, raw, raw_other), out_ref in ((refs[:3], refs[6]), (refs[3:6], refs[7])):
        half = raw.shape[1]
        for core, part in ((info[1], raw), (1 - info[1], raw_other)):
            at = pl.ds(pl.multiple_of(core * half, 128), half)
            out_ref[:, at] = mean[:, at] - scale * part[...]


def mean_step(info, one, two, up, down, entries):
    return pl.pallas_call(
        functools.partial(step_kernel, entries),
        out_shape=[jax.ShapeDtypeStruct(up[0].shape, jnp.float32)] * 2,
        in_specs=[SMEM] + [VMEM] * 8,
        out_specs=[VMEM] * 2,
        compiler_params=LIMIT,
        name="mean_step",
    )(info, one, two, *up, *down)


def halves_kernel(info, grad, w_ref, near_ref, far_ref):
    rows = near_ref.shape[1] // 2
    for bit, out_ref in ((2, far_ref), (0, near_ref)):
        for j in range(2):
            at = pl.multiple_of((info[3] ^ bit ^ j) * rows, rows)
            out_ref[:, j * rows : (j + 1) * rows] = contract_cols(
                grad[...], w_ref[pl.ds(at, rows), :]
            )


def input_halves(info, grad, w_up):
    tokens, depth = grad.shape[0], w_up.shape[0]
    return pl.pallas_call(
        halves_kernel,
        out_shape=[jax.ShapeDtypeStruct((tokens, depth // 2), jnp.float32)] * 2,
        in_specs=[SMEM] + [VMEM] * 2,
        out_specs=[VMEM] * 2,
        compiler_params=LIMIT,
        name="ig_halves",
    )(info, grad, w_up)


def after(value, earlier):
    return lax.optimization_barrier((value, earlier))[0]


def pad_images(value, images, slot):
    value = value.reshape(images, PATCHES, value.shape[-1])
    return jnp.pad(value, ((0, 0), (0, slot - PATCHES), (0, 0))).reshape(images * slot, -1)


def quad_sum(value, axis):
    pairs = [(j * 2 + core, (j ^ (1 + core)) * 2 + core) for j in range(4) for core in range(2)]
    near = lax.ppermute(value, (axis, "mc"), pairs)
    far = swap_bit(value, axis, 3)
    return value + far + near, swap_core(near)


def all_sum(value):
    one, two = quad_sum(value + swap_core(value), "mp")
    return quad_sum(one + two, "dp")


def join_kernel(info, own, other, out_ref):
    half = own.shape[1]
    for core, part in ((info[1], own), (1 - info[1], other)):
        out_ref[:, pl.ds(pl.multiple_of(core * half, 128), half)] = part[...]


def join(info, own, other):
    return pl.pallas_call(
        join_kernel,
        out_shape=jax.ShapeDtypeStruct((own.shape[0], 2 * own.shape[1]), jnp.float32),
        in_specs=[SMEM] + [VMEM] * 2,
        out_specs=VMEM,
        compiler_params=LIMIT,
    )(info, own, other)


def rows_kernel(images, slot, one, two, out_ref):
    total = one[...] + two[...]
    for image in range(images):
        piece = total[image * slot : (image + 1) * slot].T
        out_ref[:, image * PATCHES : (image + 1) * PATCHES] = piece[:, :PATCHES].astype(
            out_ref.dtype
        )


def join_rows(one, two, images, slot):
    return pl.pallas_call(
        functools.partial(rows_kernel, images, slot),
        out_shape=jax.ShapeDtypeStruct((one.shape[1], images * PATCHES), jnp.bfloat16),
        in_specs=[VMEM] * 2,
        out_specs=VMEM,
        compiler_params=LIMIT,
        name="ig_join",
    )(one, two).T[None]


def shards_line(*args):
    return line_step(*args)


def line_step(
    features, out_cotangent, mean_up, precision_up, noise_up, mean_down, precision_down, noise_down
):
    n = lax.axis_size("dp")
    me, place, core = lax.axis_index("dp"), lax.axis_index("mp"), lax.axis_index("mc")
    images = features.shape[0] // PATCHES
    slot = SLOT
    rows, width = mean_up.shape
    half = width // 2
    reach = jnp.where(me & 1, me, n - 1 - me)
    inner = (me > 0) & (me < n - 1)
    info = jnp.stack([reach, core, inner, place ^ me]).astype(jnp.int32)

    def gather(shard, first=None):
        ones, twos = [], []
        for stage in range(1, n):
            from_one, from_two = (ones[-1], twos[-1]) if ones else (shard, shard)
            if stage == 2 and first is not None:
                from_one, from_two = after((from_one, from_two), first)
            ones.append(exchange_one(from_two))
            if stage < n - 1:
                twos.append(exchange_two(from_one))
        return shard, ones, twos

    feats_raw, cot_raw = slots(features, rows), slots(out_cotangent[0], rows)
    feats, cot = pad_images(feats_raw, images, slot), pad_images(cot_raw, images, slot)
    feats_left = pad_images(feats_raw, images, DEPTH).T
    cot_left = pad_images(cot_raw, images, DEPTH).T
    shard_up = sample_weights(mean_up, precision_up, noise_up[0])
    gathered_up = [gather(shard_up, (feats, cot, feats_left, cot_left))]
    later_mean = after(mean_down, shard_up)
    gathered_down = [
        gather(sample_weights(later_mean[:, at], precision_down[:, at], noise_down[0][:, at]))
        for at in (slice(0, half), slice(half, width))
    ]

    cot_left_other = swap_core(cot_left)

    w_up, hidden, hidden_send, slope = up_stage(info, gathered_up, feats, width)
    hidden_other = swap_core(hidden_send)
    sums_down = image_sums(cot_left, cot_left_other, hidden, hidden_other, images, slot, n)
    totals_down = scatter_line(info, sums_down, n)

    preact_grad, grad_send = down_stage(info, gathered_down, cot, slope)
    grad_other = swap_core(grad_send)
    sums_up = image_sums(feats_left, feats_left, preact_grad, grad_other, images, slot, n)
    totals_up = scatter_line(info, sums_up, n)

    near_half, far_half = input_halves(info, preact_grad, w_up)
    near_half = near_half + swap_bit(far_half, "mp", 2)
    near = swap_bit(near_half[:, rows:], "mp", 1)
    input_grad = join_rows(near_half[:, :rows], near, images, slot)

    samples = lax.axis_size("mc")
    images_all = images * n

    new_down, raw_down, part = finish(info, precision_down, totals_down, (), samples, images_all)
    all_new_down = join(info, new_down, swap_core(new_down))
    raw_down_other = swap_core(raw_down)
    new_up, raw_up, part = finish(info, precision_up, totals_up, (part,), samples, images_all)
    all_new_up = join(info, new_up, swap_core(new_up))
    one, two = all_sum(part)
    raw_up_other = swap_core(raw_up)
    entries = 2 * rows * width * n * lax.axis_size("mp")
    new_mean_up, new_mean_down = mean_step(
        info,
        one,
        two,
        (mean_up, raw_up, raw_up_other),
        (mean_down, raw_down, raw_down_other),
        entries,
    )
    return new_mean_up, all_new_up, new_mean_down, all_new_down, input_grad


def solution(mesh):
    in_specs = (
        P("dp", None),
        P("mc", "dp", None),
        P("dp", "mp"),
        P("dp", "mp"),
        P("mc", "dp", "mp"),
        P("dp", "mp"),
        P("dp", "mp"),
        P("mc", "dp", "mp"),
    )
    out_specs = (P("dp", "mp"), P("dp", "mp"), P("dp", "mp"), P("dp", "mp"), P("mc", "dp", "mp"))
    sizes = mesh.shape
    line = sizes["dp"] == 4 and sizes["mp"] == 4 and sizes["mc"] == 2
    body = shards_line if line else shards_general
    return jax.shard_map(body, mesh=mesh, in_specs=in_specs, out_specs=out_specs, check_vma=False)
```
